32 devices in a mesh: row: 16 (over z, y, x), col: 2 (over core).
Axes of the slice: x: 2, y: 2, z: 4, core: 2. Of those that a mesh axis runs over, the one named last changes fastest.
Arguments:
- messages: float32 [32, 16, 2, 16, 128], P(('row', 'col')), may hold values from -6 to 6
- dst_local: int32 [32, 16, 2, 16], P(('row', 'col')), may hold values from 0 to 255
- counts: int32 [32, 16, 2], P(('row', 'col')), may hold values from 8 to 16, as said below
- degrees: int32 [8192], P(('row', 'col')), may hold values from 1 to 8
Outputs:
- aggregate: float32 [8192, 128], P(('row', 'col'))
The draws below stay inside these ranges and needn't reach their ends.
Inputs may be any that keep to these rules, and one draw needn't show every extreme that they name: For every sender and group, the counts over the group's 2 ranges sum to exactly 24. In each group one range receives 16 live slots from every sender.
All inputs are finite; a program needn't handle non-finite values.
Results may differ from the reference program's by a relative error of at most 0.0003.
Values sent between devices are 32-bit elements; how exact they have to be, the bound alone decides.
A program may use at most 64 MiB of HBM per device.

```python
import math
import jax
import jax.numpy as jnp
import numpy as np
from jax import lax

W = 128
V_DEV = 256
CAPC = 16
GROUPS = 16
SUBS = 2
SENDERS = 32
VERTICES = 8192


def draw_counts(key, part):
    first, second = jax.random.split(jax.random.fold_in(key, 11), 2)
    half = CAPC // 2
    dropped = SUBS * half // 2
    tokens = max((SUBS - 1) * half, 1)
    hot = jax.random.randint(first, (GROUPS,), 0, SUBS)
    keys = jax.random.split(second, SENDERS * GROUPS)
    perms = jax.vmap(lambda k: jax.random.permutation(k, tokens))(keys)
    chosen = (perms < dropped).astype(jnp.int32)
    owner = jnp.arange(tokens) // max(half, 1)
    onehot = (owner[:, None] == jnp.arange(SUBS - 1)[None, :]).astype(jnp.int32)
    loss_other = jnp.dot(chosen, onehot).reshape(SENDERS, GROUPS, SUBS - 1)
    ranges = jnp.arange(SUBS)
    hot_b = hot[None, :, None]
    other_index = jnp.where(ranges[None, None, :] < hot_b, ranges[None, None, :], ranges[None, None, :] - 1)
    other_index = jnp.clip(other_index, 0, SUBS - 2)
    picked = jnp.take_along_axis(loss_other, jnp.broadcast_to(other_index, (SENDERS, GROUPS, SUBS)), axis=2)
    loss = jnp.where(ranges[None, None, :] == hot_b, 0, picked)
    return (CAPC - loss).astype(jnp.int32)


def set_ends(entries, own_key, low, high):
    dims = entries.shape
    place = [jax.random.randint(jax.random.fold_in(own_key, axis), (), 0, dims[axis]) for axis in range(len(dims))]
    entries = entries.at[tuple(place)].set(low)
    longest = dims.index(max(dims))
    place[longest] = (place[longest] + 1) % dims[longest]
    return entries.at[tuple(place)].set(high)


def levels(key, shape, shards, least, high):
    def one(axis_at, blocks):
        steps = jax.random.uniform(jax.random.fold_in(jax.random.fold_in(key, 6), axis_at), (blocks,), jnp.float32, least / len(shards), high / len(shards))
        return jnp.repeat(jnp.exp(steps), shape[axis_at] // blocks).reshape((-1,) + (1,) * (len(shape) - axis_at - 1))

    level = one(*shards[0])
    for cut in shards[1:]:
        level = level * one(*cut)
    return level


def cumulative_ranks(amount, lean):
    portions = [(1 << 20) // math.isqrt(grade ** lean) + 1 for grade in range(1, amount + 1)]
    width = 1 + sum(portions) // (1 << 30)
    return np.cumsum(np.array([max(1, weight // width) for weight in portions]))


def ranked(key, extent, count, slope):
    listing = cumulative_ranks(count, slope)
    lot = jax.random.randint(jax.random.fold_in(key, 1), extent, 0, int(listing[count - 1]))
    grade = jnp.searchsorted(jnp.asarray(listing, jnp.int32), lot, side="right")
    return jax.random.permutation(jax.random.fold_in(key, 2), count)[grade].astype(jnp.int32)


def centred(stream_key, shape, spread, limit, shards=(), held_as=jnp.bfloat16):
    array = jax.random.normal(stream_key, shape, jnp.float32) * spread
    if len(shards) > 0:
        array = levels(stream_key, shape, shards, -0.22, 0.18) * array
    return jnp.clip(array, min=-limit, max=limit).astype(held_as)


def setup_inputs(seed: int = 0) -> dict:
    streams_of = jax.random.split(jax.random.key(seed), 5)
    return {
        "messages": centred(streams_of[0], (SENDERS, GROUPS, SUBS, CAPC, W), 1.0, 6.0, ((0, 32),), jnp.float32),
        "dst_local": set_ends(ranked(streams_of[1], (SENDERS, GROUPS, SUBS, CAPC), V_DEV, 2), jax.random.fold_in(streams_of[1], 3), 0, V_DEV - 1).astype(jnp.int32),
        "counts": draw_counts(jax.random.fold_in(streams_of[4], 71), 0),
        "degrees": set_ends(jax.random.randint(streams_of[3], (VERTICES,), 1, 9), jax.random.fold_in(streams_of[3], 1), 1, 8).astype(jnp.int32),
    }


def reference(messages, dst_local, counts, degrees):
    slot_index = jnp.arange(CAPC).astype(jnp.int32)
    group_index = jnp.arange(GROUPS).astype(jnp.int32)[:, None, None]
    range_index = jnp.arange(SUBS).astype(jnp.int32)[None, :, None]

    def accumulate(running, element):
        block, targets_local, count_block = element
        alive_mask = (slot_index[None, None, :] < count_block[:, :, None]).astype(jnp.float32)
        target = ((group_index * SUBS + range_index) * V_DEV + targets_local).astype(jnp.int32)
        values = block * alive_mask[..., None]
        running = running.at[target.reshape(-1)].add(values.reshape(-1, W))
        return running, None

    start = jnp.zeros((VERTICES, W), jnp.float32)
    summed, _ = lax.scan(accumulate, start, (messages, dst_local, counts))
    scale = jnp.maximum(degrees, 1).astype(jnp.float32)
    return summed / scale[:, None]
```

```python
import functools

import jax
import jax.numpy as jnp
from jax import lax
from jax.experimental import pallas as pl
from jax.experimental.pallas import tpu as pltpu
from jax.sharding import PartitionSpec as P

MESH = pl.DeviceIdType.MESH
LANES = 128


def exchange(rows, cols, msg_ref, dst_ref, cnt_ref, out_ref, stage, recv, labels, copy_sem, send_sem, recv_sem):
    slots = msg_ref.shape[1]
    owned = out_ref.shape[0]
    total = rows * cols
    pack = LANES // slots
    planes = total // pack
    half = max(planes // 2, 1)
    me = lax.axis_index("row") * cols + lax.axis_index("col")
    plane, seat = me // pack, me % pack
    side = plane // half
    mirrored = plane * (1 - side) + (planes - 1 - plane) * side

    load = pltpu.make_async_copy(msg_ref, stage.at[:, pl.ds(0, slots), :], copy_sem.at[0])
    load.start()

    def partner(step, j):
        if planes > 1:
            ahead = planes - 1 - step if step < half else (mirrored + planes - 1 - step) % half
            there = ahead * (1 - side) + (planes - 1 - ahead) * side
        else:
            there = 0
        return there * pack + (seat + j) % pack

    def each(visit):
        for step in range(planes):
            first = 1 if step == planes - 1 else 0
            if total <= 64:
                for j in range(first, pack):
                    visit(partner(step, j))
            else:
                lax.fori_loop(first, pack, lambda j, c, step=step: (visit(partner(step, j)), c)[1], 0)

    barrier = pltpu.get_barrier_semaphore()
    each(lambda t: pl.semaphore_signal(barrier, inc=1, device_id=(t // cols, t % cols), device_id_type=MESH))

    lane = lax.broadcasted_iota(jnp.int32, (cols, slots), 1)
    row = lax.broadcasted_iota(jnp.int32, (cols, slots), 0)
    labels[...] = jnp.zeros_like(labels)
    for g in range(rows):
        live = jnp.zeros((cols, slots), jnp.int32)
        for c in range(cols):
            live = jnp.where(row == c, cnt_ref[c, g], live)
        value = jnp.where(lane < live, dst_ref[0, g], -1)
        labels[pl.ds(g * cols, cols), pl.ds(0, slots)] = value.astype(jnp.float32)
    rolled = pltpu.roll(labels[...], seat * slots, 1)
    stage[:, slots, :] = rolled
    load.wait()
    own = pltpu.make_async_copy(stage.at[me], recv.at[me], recv_sem.at[plane])

    pl.semaphore_wait(barrier, total - 1)

    def send(t):
        pltpu.make_async_remote_copy(
            src_ref=stage.at[t],
            dst_ref=recv.at[me],
            send_sem=send_sem,
            recv_sem=recv_sem.at[plane],
            device_id=(t // cols, t % cols),
            device_id_type=MESH,
        ).start()

    each(send)
    own.start()

    vertex = lax.broadcasted_iota(jnp.int32, (owned, LANES), 0).astype(jnp.float32)
    width = msg_ref.shape[2]

    def block(q, acc):
        part = recv.at[pl.ds(q * pack, pack)]
        pltpu.make_async_copy(part, part, recv_sem.at[q]).wait()
        label = jnp.sum(recv[pl.ds(q * pack, pack), slots, :], axis=0, keepdims=True)
        hot = (vertex == label).astype(jnp.bfloat16)
        values = recv[pl.ds(q * pack, pack), pl.ds(0, slots), :].reshape(pack * slots, width)
        high = values.astype(jnp.bfloat16)
        low = (values - high.astype(jnp.float32)).astype(jnp.bfloat16)
        both = jnp.concatenate([high, low], axis=1)
        return acc + jnp.dot(hot, both, preferred_element_type=jnp.float32)

    acc = jnp.zeros((owned, 2 * width), jnp.float32)
    if planes <= 8:
        for d in range(planes):
            acc = block((plane + d) % planes, acc)
    else:
        acc = lax.fori_loop(0, planes, lambda d, a: block((plane + d) % planes, a), acc)
    out_ref[...] = acc[:, :width] + acc[:, width:]
    sent = stage.at[pl.ds(0, total - 1)]
    pltpu.make_async_copy(sent, sent, send_sem).wait()


def solution(mesh):
    rows, cols = mesh.shape["row"], mesh.shape["col"]
    total = rows * cols

    def body(messages, dst_local, counts, degrees):
        slots, width = messages.shape[3:]
        owned = degrees.shape[0]
        planes = total // (LANES // slots)
        summed = pl.pallas_call(
            functools.partial(exchange, rows, cols),
            out_shape=jax.ShapeDtypeStruct((owned, width), jnp.float32),
            in_specs=[
                pl.BlockSpec(memory_space=pl.ANY),
                pl.BlockSpec(memory_space=pltpu.VMEM),
                pl.BlockSpec(memory_space=pltpu.SMEM),
            ],
            out_specs=pl.BlockSpec(memory_space=pltpu.VMEM),
            scratch_shapes=[
                pltpu.VMEM((total, slots + 1, width), jnp.float32),
                pltpu.VMEM((total, slots + 1, width), jnp.float32),
                pltpu.VMEM((total, LANES), jnp.float32),
                pltpu.SemaphoreType.DMA((1,)),
                pltpu.SemaphoreType.DMA,
                pltpu.SemaphoreType.DMA((planes,)),
            ],
            compiler_params=pltpu.CompilerParams(collective_id=0, has_side_effects=True),
        )(messages.reshape(total, slots, width), dst_local, counts[0].T)
        scale = jnp.maximum(degrees, 1).astype(jnp.float32)
        return summed / scale[:, None]

    in_specs = (
        P(("row", "col"), None, None, None, None),
        P(("row", "col"), None, None, None),
        P(("row", "col"), None, None),
        P(("row", "col")),
    )
    return jax.shard_map(body, mesh=mesh, in_specs=in_specs, out_specs=P(("row", "col"), None), check_vma=False)
```

```python
import functools

import jax
import jax.numpy as jnp
from jax import lax
from jax.experimental import pallas as pl
from jax.experimental.pallas import tpu as pltpu
from jax.sharding import PartitionSpec as P

MESH = pl.DeviceIdType.MESH
LANES = 128


def exchange(rows, cols, msg_ref, dst_ref, cnt_ref, out_ref, stage, recv, labels, dst, cnt, copy_sem, send_sem, recv_sem, up_sem):
    slots, width = msg_ref.shape[1:]
    owned = out_ref.shape[0]
    total = rows * cols
    pack = LANES // slots
    planes = total // pack
    me = lax.axis_index("row") * cols + lax.axis_index("col")
    plane, seat = me // pack, me % pack

    def device(t):
        return (t // cols, t % cols)

    def repeat(first, last, visit):
        if last - first <= 8:
            for i in range(first, last):
                visit(i)
        else:
            lax.fori_loop(first, last, lambda i, c: (visit(i), c)[1], 0)

    barrier = pltpu.get_barrier_semaphore()

    def greet(t):
        pl.semaphore_signal(barrier, inc=1, device_id=device(t), device_id_type=MESH)

    repeat(1, pack, lambda j: greet(plane * pack + (seat + j) % pack))
    has_below = plane > 0
    has_above = plane < planes - 1

    @pl.when(has_below)
    def _():
        greet(me - pack)

    @pl.when(has_above)
    def _():
        greet(me + pack)

    loads = [
        pltpu.make_async_copy(dst_ref, dst, copy_sem.at[0]),
        pltpu.make_async_copy(cnt_ref, cnt, copy_sem.at[1]),
        pltpu.make_async_copy(msg_ref, stage.at[:, pl.ds(0, slots), :], copy_sem.at[2]),
    ]
    for load in loads:
        load.start()
    labels[...] = jnp.zeros_like(labels)
    loads[0].wait()
    loads[1].wait()

    lane = lax.broadcasted_iota(jnp.int32, (cols, slots), 1)
    for g in range(rows):
        value = jnp.where(lane < cnt[:, g : g + 1], dst[0, g], -1)
        labels[pl.ds(g * cols, cols), pl.ds(0, slots)] = value.astype(jnp.float32)
    stage[:, slots, :] = pltpu.roll(labels[...], seat * slots, 1)
    loads[2].wait()

    def tell(q, t):
        pl.semaphore_signal(up_sem.at[q], inc=1, device_id=device(t), device_id_type=MESH)

    def send(t):
        pltpu.make_async_remote_copy(
            src_ref=stage.at[t],
            dst_ref=recv.at[me],
            send_sem=send_sem,
            recv_sem=recv_sem.at[plane],
            device_id=device(t),
            device_id_type=MESH,
        ).start()

    pl.semaphore_wait(barrier, pack + 1 - (planes - plane) // planes - (plane + 1) // planes)

    @pl.when(has_below)
    def _():
        tell(plane, me - pack)

    @pl.when(has_above)
    def _():
        tell(plane, me + pack)

    repeat(1, pack, lambda j: send(plane * pack + (seat + j) % pack))
    own = pltpu.make_async_copy(stage.at[me], recv.at[me], recv_sem.at[plane])
    own.start()

    def other(i):
        lower = (planes + plane - 1 - i) // planes
        return lower, lower * (plane - 1 - i) + (1 - lower) * (i + 1)

    def forward(i):
        lower, q = other(i)
        pl.semaphore_wait(up_sem.at[q], 1)
        onward = plane + 2 * lower - 1

        @pl.when((onward >= 0) & (onward < planes))
        def _():
            tell(q, onward * pack + seat)

        repeat(0, pack, lambda j: send(q * pack + (seat + j) % pack))

    repeat(0, planes - 1, forward)

    vertex = lax.broadcasted_iota(jnp.int32, (owned, LANES), 0).astype(jnp.float32)

    def block(q, acc):
        part = recv.at[pl.ds(q * pack, pack)]
        pltpu.make_async_copy(part, part, recv_sem.at[q]).wait()
        label = jnp.sum(recv[pl.ds(q * pack, pack), slots, :], axis=0, keepdims=True)
        hot = (vertex == label).astype(jnp.bfloat16)
        values = recv[pl.ds(q * pack, pack), pl.ds(0, slots), :].reshape(pack * slots, width)
        high = values.astype(jnp.bfloat16)
        low = (values - high.astype(jnp.float32)).astype(jnp.bfloat16)
        both = jnp.concatenate([high, low], axis=1)
        return acc + jnp.dot(hot, both, preferred_element_type=jnp.float32)

    acc = block(plane, jnp.zeros((owned, 2 * width), jnp.float32))
    if planes <= 8:
        for i in range(planes - 1):
            acc = block(other(i)[1], acc)
    else:
        acc = lax.fori_loop(0, planes - 1, lambda i, a: block(other(i)[1], a), acc)
    out_ref[...] = acc[:, :width] + acc[:, width:]
    sent = stage.at[pl.ds(0, total - 1)]
    pltpu.make_async_copy(sent, sent, send_sem).wait()


def solution(mesh):
    rows, cols = mesh.shape["row"], mesh.shape["col"]
    total = rows * cols

    def body(messages, dst_local, counts, degrees):
        slots, width = messages.shape[3:]
        owned = degrees.shape[0]
        planes = total // (LANES // slots)
        summed = pl.pallas_call(
            functools.partial(exchange, rows, cols),
            out_shape=jax.ShapeDtypeStruct((owned, width), jnp.float32),
            in_specs=[
                pl.BlockSpec(memory_space=pl.ANY),
                pl.BlockSpec(memory_space=pl.ANY),
                pl.BlockSpec(memory_space=pl.ANY),
            ],
            out_specs=pl.BlockSpec(memory_space=pltpu.VMEM),
            scratch_shapes=[
                pltpu.VMEM((total, slots + 1, width), jnp.float32),
                pltpu.VMEM((total, slots + 1, width), jnp.float32),
                pltpu.VMEM((total, LANES), jnp.float32),
                pltpu.VMEM(dst_local.shape, jnp.int32),
                pltpu.VMEM((cols, rows), jnp.int32),
                pltpu.SemaphoreType.DMA((3,)),
                pltpu.SemaphoreType.DMA,
                pltpu.SemaphoreType.DMA((planes,)),
                pltpu.SemaphoreType.REGULAR((planes,)),
            ],
            compiler_params=pltpu.CompilerParams(collective_id=0, has_side_effects=True),
        )(messages.reshape(total, slots, width), dst_local, counts[0].T)
        summed, degrees = lax.optimization_barrier((summed, degrees))
        scale = jnp.maximum(degrees, 1).astype(jnp.float32)
        return summed / scale[:, None]

    in_specs = (
        P(("row", "col"), None, None, None, None),
        P(("row", "col"), None, None, None),
        P(("row", "col"), None, None),
        P(("row", "col")),
    )
    return jax.shard_map(body, mesh=mesh, in_specs=in_specs, out_specs=P(("row", "col"), None), check_vma=False)
```

```python
import functools

import jax
import jax.numpy as jnp
from jax import lax
from jax.experimental import pallas as pl
from jax.experimental.pallas import tpu as pltpu
from jax.sharding import PartitionSpec as P

MESH = pl.DeviceIdType.MESH
LANES = 128


def exchange(rows, cols, msg_ref, dst_ref, cnt_ref, deg_ref, out_ref, deg, stage, recv, labels, dst, cnt, copy_sem, send_sem, recv_sem, up_sem):
    slots, width = msg_ref.shape[1:]
    owned = out_ref.shape[0]
    total = rows * cols
    pack = LANES // slots
    planes = total // pack
    me = lax.axis_index("row") * cols + lax.axis_index("col")
    plane, seat = me // pack, me % pack

    def device(t):
        return (t // cols, t % cols)

    def repeat(first, last, visit):
        if last - first <= 8:
            for i in range(first, last):
                visit(i)
        else:
            lax.fori_loop(first, last, lambda i, c: (visit(i), c)[1], 0)

    loads = [
        pltpu.make_async_copy(dst_ref, dst, copy_sem.at[0]),
        pltpu.make_async_copy(cnt_ref, cnt, copy_sem.at[1]),
        pltpu.make_async_copy(deg_ref, deg, copy_sem.at[3]),
        pltpu.make_async_copy(msg_ref, stage.at[:, pl.ds(0, slots), :], copy_sem.at[2]),
    ]
    for load in loads:
        load.start()
    barrier = pltpu.get_barrier_semaphore()

    def greet(t):
        pl.semaphore_signal(barrier, inc=1, device_id=device(t), device_id_type=MESH)

    def greet_above(d):
        @pl.when(plane + d < planes)
        def _():
            repeat(0, pack, lambda j: greet((plane + d) * pack + (seat + j) % pack))

    repeat(1, pack, lambda j: greet(plane * pack + (seat + j) % pack))
    repeat(1, planes, greet_above)
    labels[...] = jnp.zeros_like(labels)
    loads[0].wait()
    loads[1].wait()

    lane = lax.broadcasted_iota(jnp.int32, (cols, slots), 1)
    for g in range(rows):
        value = jnp.where(lane < cnt[:, g : g + 1], dst[0, g], -1)
        labels[pl.ds(g * cols, cols), pl.ds(0, slots)] = value.astype(jnp.float32)
    stage[:, slots, :] = pltpu.roll(labels[...], seat * slots, 1)
    loads[2].wait()
    loads[3].wait()
    size = deg.shape[1]
    same = lax.broadcasted_iota(jnp.int32, (size, size), 0) == lax.broadcasted_iota(jnp.int32, (size, size), 1)
    scale = jnp.concatenate(
        [jnp.sum(jnp.where(same, jnp.maximum(deg[i : i + 1, :], 1), 0).astype(jnp.float32), axis=1, keepdims=True) for i in range(deg.shape[0])],
        axis=0,
    )

    def send(t):
        pltpu.make_async_remote_copy(
            src_ref=stage.at[t],
            dst_ref=recv.at[me],
            send_sem=send_sem,
            recv_sem=recv_sem.at[plane],
            device_id=device(t),
            device_id_type=MESH,
        ).start()

    pl.semaphore_wait(barrier, pack - 1 + pack * plane)

    def tell_below(d):
        @pl.when(plane - d >= 0)
        def _():
            t = me - d * pack
            pl.semaphore_signal(up_sem.at[plane], inc=1, device_id=device(t), device_id_type=MESH)

    def send_below(i):
        d = planes - i

        @pl.when(plane - d >= 0)
        def _():
            repeat(0, pack, lambda j: send((plane - d) * pack + j))

    def send_above(d):
        @pl.when(plane + d < planes)
        def _():
            pl.semaphore_wait(up_sem.at[plane + d], 1)
            repeat(0, pack, lambda j: send((plane + d) * pack + j))

    repeat(1, planes, tell_below)
    repeat(1, planes, send_below)
    repeat(1, pack, lambda j: send(plane * pack + (seat + j) % pack))
    own = pltpu.make_async_copy(stage.at[me], recv.at[me], recv_sem.at[plane])
    own.start()
    repeat(1, planes, send_above)

    def other(i):
        lower = (planes + plane - 1 - i) // planes
        return lower * (plane - 1 - i) + (1 - lower) * (i + 1)

    vertex = lax.broadcasted_iota(jnp.int32, (owned, LANES), 0).astype(jnp.float32)

    def block(q, acc):
        part = recv.at[pl.ds(q * pack, pack)]
        pltpu.make_async_copy(part, part, recv_sem.at[q]).wait()
        label = jnp.sum(recv[pl.ds(q * pack, pack), slots, :], axis=0, keepdims=True)
        hot = (vertex == label).astype(jnp.bfloat16)
        values = recv[pl.ds(q * pack, pack), pl.ds(0, slots), :].reshape(pack * slots, width)
        high = values.astype(jnp.bfloat16)
        low = (values - high.astype(jnp.float32)).astype(jnp.bfloat16)
        both = jnp.concatenate([high, low], axis=1)
        return acc + jnp.dot(hot, both, preferred_element_type=jnp.float32)

    acc = block(plane, jnp.zeros((owned, 2 * width), jnp.float32))
    if planes <= 8:
        for i in range(planes - 1):
            acc = block(other(i), acc)
    else:
        acc = lax.fori_loop(0, planes - 1, lambda i, a: block(other(i), a), acc)
    out_ref[...] = (acc[:, :width] + acc[:, width:]) / scale
    sent = stage.at[pl.ds(0, total - 1)]
    pltpu.make_async_copy(sent, sent, send_sem).wait()


def solution(mesh):
    rows, cols = mesh.shape["row"], mesh.shape["col"]
    total = rows * cols

    def body(messages, dst_local, counts, degrees):
        slots, width = messages.shape[3:]
        owned = degrees.shape[0]
        planes = total // (LANES // slots)
        summed = pl.pallas_call(
            functools.partial(exchange, rows, cols),
            out_shape=pltpu.VMEM((owned, width), jnp.float32),
            in_specs=[
                pl.BlockSpec(memory_space=pl.ANY),
                pl.BlockSpec(memory_space=pl.ANY),
                pl.BlockSpec(memory_space=pl.ANY),
                pl.BlockSpec(memory_space=pl.ANY),
            ],
            out_specs=pl.BlockSpec(memory_space=pltpu.VMEM),
            scratch_shapes=[
                pltpu.VMEM((owned // LANES, LANES), jnp.int32),
                pltpu.VMEM((total, slots + 1, width), jnp.float32),
                pltpu.VMEM((total, slots + 1, width), jnp.float32),
                pltpu.VMEM((total, LANES), jnp.float32),
                pltpu.VMEM(dst_local.shape, jnp.int32),
                pltpu.VMEM((cols, rows), jnp.int32),
                pltpu.SemaphoreType.DMA((4,)),
                pltpu.SemaphoreType.DMA,
                pltpu.SemaphoreType.DMA((planes,)),
                pltpu.SemaphoreType.REGULAR((planes,)),
            ],
            compiler_params=pltpu.CompilerParams(collective_id=0, has_side_effects=True),
        )(messages.reshape(total, slots, width), dst_local, counts[0].T, degrees.reshape(-1, LANES))
        return summed

    in_specs = (
        P(("row", "col"), None, None, None, None),
        P(("row", "col"), None, None, None),
        P(("row", "col"), None, None),
        P(("row", "col")),
    )
    return jax.shard_map(body, mesh=mesh, in_specs=in_specs, out_specs=P(("row", "col"), None), check_vma=False)
```

```python
import functools

import jax
import jax.numpy as jnp
from jax import lax
from jax.experimental import pallas as pl
from jax.experimental.pallas import tpu as pltpu
from jax.sharding import PartitionSpec as P

MESH = pl.DeviceIdType.MESH
LANES = 128


def exchange(rows, cols, msg_ref, dst_ref, cnt_ref, deg_ref, out_ref, deg, stage, recv, labels, dst, cnt, spare, copy_sem, send_sem, recv_sem, up_sem, extra_sem, pass_sem, tail_sem):
    slots, width = msg_ref.shape[1:]
    owned = out_ref.shape[0]
    total = rows * cols
    pack = LANES // slots
    planes = total // pack
    me = lax.axis_index("row") * cols + lax.axis_index("col")
    plane, seat = me // pack, me % pack
    core = lax.axis_index("col")
    paired = cols == 2 and slots % 16 == 0
    cut = slots // 2 if paired else 0
    pairs = pack // cols

    def device(t):
        return (t // cols, t % cols)

    def repeat(first, last, visit):
        if last - first <= 8:
            for i in range(first, last):
                visit(i)
        else:
            lax.fori_loop(first, last, lambda i, c: (visit(i), c)[1], 0)

    loads = [
        pltpu.make_async_copy(dst_ref, dst, copy_sem.at[0]),
        pltpu.make_async_copy(cnt_ref, cnt, copy_sem.at[1]),
        pltpu.make_async_copy(deg_ref, deg, copy_sem.at[3]),
        pltpu.make_async_copy(msg_ref.at[:, pl.ds(0, slots - cut)], stage.at[:, pl.ds(cut, slots - cut), :], copy_sem.at[2]),
    ]
    if paired:
        loads.append(pltpu.make_async_copy(msg_ref.at[:, pl.ds(cut, cut)], spare, copy_sem.at[4]))
    for load in loads:
        load.start()
    barrier = pltpu.get_barrier_semaphore()

    def greet(t):
        pl.semaphore_signal(barrier, inc=1, device_id=device(t), device_id_type=MESH)

    def greet_above(d):
        @pl.when(plane + d < planes)
        def _():
            repeat(0, pack, lambda j: greet((plane + d) * pack + (seat + j) % pack))

    repeat(1, pack, lambda j: greet(plane * pack + (seat + j) % pack))
    repeat(1, planes, greet_above)
    labels[...] = jnp.zeros_like(labels)
    loads[0].wait()
    loads[1].wait()

    lane = lax.broadcasted_iota(jnp.int32, (cols, slots), 1)
    base = lax.broadcasted_iota(jnp.int32, (cols, slots), 0) * owned
    for g in range(rows):
        value = jnp.where(lane < cnt[:, g : g + 1], dst[0, g] + base, -1).astype(jnp.float32)
        if paired:
            second = cnt[1:2, g : g + 1] > cnt[0:1, g : g + 1]
            extra = jnp.where(second, value[1:2, cut:], value[0:1, cut:])
            labels[pl.ds(g * cols, cols), pl.ds(0, cut)] = jnp.broadcast_to(extra, (cols, cut))
            labels[pl.ds(g * cols, cols), pl.ds(cut, cut)] = value[:, :cut]
        else:
            labels[pl.ds(g * cols, cols), pl.ds(0, slots)] = value
    stage[:, slots, :] = pltpu.roll(labels[...], seat * slots, 1)
    loads[2].wait()
    loads[3].wait()
    if paired:
        loads[4].wait()
        for g in range(rows):
            second = cnt[1:2, g : g + 1] > cnt[0:1, g : g + 1]
            stage[g, pl.ds(0, cut), :] = jnp.where(second, spare[g * cols + 1], spare[g * cols])
    size = deg.shape[1]
    same = lax.broadcasted_iota(jnp.int32, (size, size), 0) == lax.broadcasted_iota(jnp.int32, (size, size), 1)
    scale = jnp.concatenate(
        [jnp.sum(jnp.where(same, jnp.maximum(deg[i : i + 1, :], 1), 0).astype(jnp.float32), axis=1, keepdims=True) for i in range(deg.shape[0])],
        axis=0,
    )

    body = pl.ds(cut, slots + 1 - cut)
    head = pl.ds(0, cut)

    def send(t):
        pltpu.make_async_remote_copy(
            src_ref=stage.at[t, body],
            dst_ref=recv.at[me // cols, core, body],
            send_sem=send_sem,
            recv_sem=recv_sem.at[plane],
            device_id=device(t),
            device_id_type=MESH,
        ).start()

    def send_extra(g):
        pltpu.make_async_remote_copy(
            src_ref=stage.at[g, head],
            dst_ref=recv.at[me // cols, core, head],
            send_sem=tail_sem.at[0],
            recv_sem=extra_sem.at[plane],
            device_id=(g, core),
            device_id_type=MESH,
        ).start()

    def send_plane(q):
        if paired:
            repeat(0, pairs, lambda j: send_extra(q * pairs + j))
        repeat(0, pack, lambda j: send(q * pack + j))

    pl.semaphore_wait(barrier, pack - 1 + pack * plane)

    def tell_below(d):
        @pl.when(plane - d >= 0)
        def _():
            t = me - d * pack
            pl.semaphore_signal(up_sem.at[plane], inc=1, device_id=device(t), device_id_type=MESH)

    def send_below(i):
        d = planes - i

        @pl.when(plane - d >= 0)
        def _():
            send_plane(plane - d)

    def send_above(d):
        @pl.when(plane + d < planes)
        def _():
            pl.semaphore_wait(up_sem.at[plane + d], 1)
            send_plane(plane + d)

    repeat(1, planes, tell_below)
    repeat(1, planes, send_below)
    if paired:
        repeat(1, pairs, lambda j: send_extra(plane * pairs + (seat // cols + j) % pairs))
        pltpu.make_async_copy(stage.at[me // cols, head], recv.at[me // cols, core, head], extra_sem.at[plane]).start()
    repeat(1, pack, lambda j: send(plane * pack + (seat + j) % pack))
    pltpu.make_async_copy(stage.at[me, body], recv.at[me // cols, core, body], recv_sem.at[plane]).start()
    repeat(1, planes, send_above)

    def other(i):
        lower = (planes + plane - 1 - i) // planes
        return lower * (plane - 1 - i) + (1 - lower) * (i + 1)

    def hand(q):
        part = recv.at[pl.ds(q * pairs, pairs), core, head]
        pltpu.make_async_copy(part, part, extra_sem.at[q]).wait()
        pltpu.make_async_remote_copy(
            src_ref=part,
            dst_ref=part,
            send_sem=tail_sem.at[1],
            recv_sem=pass_sem.at[q],
            device_id=(lax.axis_index("row"), 1 - core),
            device_id_type=MESH,
        ).start()

    if paired:
        hand(plane)
        repeat(0, planes - 1, lambda i: hand(other(i)))

    vertex = (lax.broadcasted_iota(jnp.int32, (owned, LANES), 0) + core * owned).astype(jnp.float32)

    def block(q, acc):
        part = recv.at[pl.ds(q * pairs, pairs), :, body]
        pltpu.make_async_copy(part, part, recv_sem.at[q]).wait()
        if paired:
            part = recv.at[pl.ds(q * pairs, pairs), 1 - core, head]
            pltpu.make_async_copy(part, part, pass_sem.at[q]).wait()
        label = jnp.sum(recv[pl.ds(q * pairs, pairs), :, slots, :].reshape(pack, width), axis=0, keepdims=True)
        hot = (vertex == label).astype(jnp.bfloat16)
        values = recv[pl.ds(q * pairs, pairs), :, pl.ds(0, slots), :].reshape(pack * slots, width)
        high = values.astype(jnp.bfloat16)
        low = (values - high.astype(jnp.float32)).astype(jnp.bfloat16)
        both = jnp.concatenate([high, low], axis=1)
        return acc + jnp.dot(hot, both, preferred_element_type=jnp.float32)

    acc = block(plane, jnp.zeros((owned, 2 * width), jnp.float32))
    if planes <= 8:
        for i in range(planes - 1):
            acc = block(other(i), acc)
    else:
        acc = lax.fori_loop(0, planes - 1, lambda i, a: block(other(i), a), acc)
    out_ref[...] = (acc[:, :width] + acc[:, width:]) / scale
    sent = stage.at[pl.ds(0, total - 1), body]
    pltpu.make_async_copy(sent, sent, send_sem).wait()
    if paired:
        for count, sem in ((rows - 1, 0), (rows, 1)):
            sent = stage.at[pl.ds(0, count), head]
            pltpu.make_async_copy(sent, sent, tail_sem.at[sem]).wait()


def solution(mesh):
    rows, cols = mesh.shape["row"], mesh.shape["col"]
    total = rows * cols

    def body(messages, dst_local, counts, degrees):
        slots, width = messages.shape[3:]
        owned = degrees.shape[0]
        planes = total // (LANES // slots)
        summed = pl.pallas_call(
            functools.partial(exchange, rows, cols),
            out_shape=pltpu.VMEM((owned, width), jnp.float32),
            in_specs=[
                pl.BlockSpec(memory_space=pl.ANY),
                pl.BlockSpec(memory_space=pl.ANY),
                pl.BlockSpec(memory_space=pl.ANY),
                pl.BlockSpec(memory_space=pl.ANY),
            ],
            out_specs=pl.BlockSpec(memory_space=pltpu.VMEM),
            scratch_shapes=[
                pltpu.VMEM((owned // LANES, LANES), jnp.int32),
                pltpu.VMEM((total, slots + 1, width), jnp.float32),
                pltpu.VMEM((rows, cols, slots + 1, width), jnp.float32),
                pltpu.VMEM((total, LANES), jnp.float32),
                pltpu.VMEM(dst_local.shape, jnp.int32),
                pltpu.VMEM((cols, rows), jnp.int32),
                pltpu.VMEM((total, slots // 2, width), jnp.float32),
                pltpu.SemaphoreType.DMA((5,)),
                pltpu.SemaphoreType.DMA,
                pltpu.SemaphoreType.DMA((planes,)),
                pltpu.SemaphoreType.REGULAR((planes,)),
                pltpu.SemaphoreType.DMA((planes,)),
                pltpu.SemaphoreType.DMA((planes,)),
                pltpu.SemaphoreType.DMA((2,)),
            ],
            compiler_params=pltpu.CompilerParams(collective_id=0, has_side_effects=True),
        )(messages.reshape(total, slots, width), dst_local, counts[0].T, degrees.reshape(-1, LANES))
        return summed

    in_specs = (
        P(("row", "col"), None, None, None, None),
        P(("row", "col"), None, None, None),
        P(("row", "col"), None, None),
        P(("row", "col")),
    )
    return jax.shard_map(body, mesh=mesh, in_specs=in_specs, out_specs=P(("row", "col"), None), check_vma=False)
```

```python
import functools

import jax
import jax.numpy as jnp
from jax import lax
from jax.experimental import pallas as pl
from jax.experimental.pallas import tpu as pltpu
from jax.sharding import PartitionSpec as P

MESH = pl.DeviceIdType.MESH
LANES = 128


def exchange(rows, cols, msg_ref, dst_ref, cnt_ref, deg_ref, out_ref, deg, stage, recv, labels, dst, cnt, spare, copy_sem, send_sem, recv_sem, up_sem, extra_sem, pass_sem, tail_sem):
    slots, width = msg_ref.shape[1:]
    owned = out_ref.shape[0]
    total = rows * cols
    pack = LANES // slots
    planes = total // pack
    me = lax.axis_index("row") * cols + lax.axis_index("col")
    plane, seat = me // pack, me % pack
    core = lax.axis_index("col")
    paired = cols == 2 and slots % 16 == 0
    cut = slots // 2 if paired else 0
    pairs = pack // cols

    def device(t):
        return (t // cols, t % cols)

    def repeat(first, last, visit):
        if last - first <= 8:
            for i in range(first, last):
                visit(i)
        else:
            lax.fori_loop(first, last, lambda i, c: (visit(i), c)[1], 0)

    loads = [
        pltpu.make_async_copy(dst_ref, dst, copy_sem.at[0]),
        pltpu.make_async_copy(cnt_ref, cnt, copy_sem.at[1]),
        pltpu.make_async_copy(deg_ref, deg, copy_sem.at[3]),
        pltpu.make_async_copy(msg_ref.at[:, pl.ds(0, slots - cut)], stage.at[:, pl.ds(cut, slots - cut), :], copy_sem.at[2]),
    ]
    if paired:
        loads.append(pltpu.make_async_copy(msg_ref.at[:, pl.ds(cut, cut)], spare, copy_sem.at[4]))
    for load in loads:
        load.start()
    barrier = pltpu.get_barrier_semaphore()

    def greet(t):
        pl.semaphore_signal(barrier, inc=1, device_id=device(t), device_id_type=MESH)

    def greet_above(d):
        @pl.when(plane + d < planes)
        def _():
            repeat(0, pack, lambda j: greet((plane + d) * pack + (seat + j) % pack))

    repeat(1, pack, lambda j: greet(plane * pack + (seat + j) % pack))
    repeat(1, planes, greet_above)
    labels[...] = jnp.zeros_like(labels)
    loads[0].wait()
    loads[1].wait()

    lane = lax.broadcasted_iota(jnp.int32, (cols, slots), 1)
    base = lax.broadcasted_iota(jnp.int32, (cols, slots), 0) * owned
    for g in range(rows):
        value = jnp.where(lane < cnt[:, g : g + 1], dst[0, g] + base, -1).astype(jnp.float32)
        if paired:
            second = cnt[1:2, g : g + 1] > cnt[0:1, g : g + 1]
            extra = jnp.where(second, value[1:2, cut:], value[0:1, cut:])
            labels[pl.ds(g * cols, cols), pl.ds(0, cut)] = jnp.broadcast_to(extra, (cols, cut))
            labels[pl.ds(g * cols, cols), pl.ds(cut, cut)] = value[:, :cut]
        else:
            labels[pl.ds(g * cols, cols), pl.ds(0, slots)] = value
    stage[:, slots, :] = pltpu.roll(labels[...], seat * slots, 1)
    loads[2].wait()
    loads[3].wait()
    if paired:
        loads[4].wait()
        for g in range(rows):
            second = cnt[1:2, g : g + 1] > cnt[0:1, g : g + 1]
            stage[g, pl.ds(0, cut), :] = jnp.where(second, spare[g * cols + 1], spare[g * cols])
    size = deg.shape[1]
    same = lax.broadcasted_iota(jnp.int32, (size, size), 0) == lax.broadcasted_iota(jnp.int32, (size, size), 1)
    scale = jnp.concatenate(
        [jnp.sum(jnp.where(same, jnp.maximum(deg[i : i + 1, :], 1), 0).astype(jnp.float32), axis=1, keepdims=True) for i in range(deg.shape[0])],
        axis=0,
    )

    body = pl.ds(cut, slots + 1 - cut)
    head = pl.ds(0, cut)

    def send(t):
        pltpu.make_async_remote_copy(
            src_ref=stage.at[t, body],
            dst_ref=recv.at[me // cols, core, body],
            send_sem=send_sem,
            recv_sem=recv_sem.at[plane],
            device_id=device(t),
            device_id_type=MESH,
        ).start()

    def send_extra(g):
        pltpu.make_async_remote_copy(
            src_ref=stage.at[g, head],
            dst_ref=recv.at[me // cols, core, head],
            send_sem=tail_sem.at[0],
            recv_sem=extra_sem.at[plane],
            device_id=(g, 1 - core),
            device_id_type=MESH,
        ).start()

    def send_plane(q):
        if paired:
            repeat(0, pairs, lambda j: send_extra(q * pairs + j))
        repeat(0, pack, lambda j: send(q * pack + j))

    pl.semaphore_wait(barrier, pack - 1 + pack * plane)

    def tell_below(d):
        @pl.when(plane - d >= 0)
        def _():
            t = me - d * pack
            pl.semaphore_signal(up_sem.at[plane], inc=1, device_id=device(t), device_id_type=MESH)

    def send_below(i):
        d = planes - i

        @pl.when(plane - d >= 0)
        def _():
            send_plane(plane - d)

    def send_above(d):
        @pl.when(plane + d < planes)
        def _():
            pl.semaphore_wait(up_sem.at[plane + d], 1)
            send_plane(plane + d)

    repeat(1, planes, tell_below)
    repeat(1, planes, send_below)
    if paired:
        repeat(0, pairs, lambda j: send_extra(plane * pairs + (seat // cols + j) % pairs))
    repeat(1, pack, lambda j: send(plane * pack + (seat + j) % pack))
    pltpu.make_async_copy(stage.at[me, body], recv.at[me // cols, core, body], recv_sem.at[plane]).start()
    repeat(1, planes, send_above)

    def other(i):
        lower = (planes + plane - 1 - i) // planes
        return lower * (plane - 1 - i) + (1 - lower) * (i + 1)

    def hand(q):
        part = recv.at[pl.ds(q * pairs, pairs), 1 - core, head]
        pltpu.make_async_copy(part, part, extra_sem.at[q]).wait()
        pltpu.make_async_remote_copy(
            src_ref=part,
            dst_ref=part,
            send_sem=tail_sem.at[1],
            recv_sem=pass_sem.at[q],
            device_id=(lax.axis_index("row"), 1 - core),
            device_id_type=MESH,
        ).start()

    if paired:
        hand(plane)
        repeat(0, planes - 1, lambda i: hand(other(i)))

    vertex = (lax.broadcasted_iota(jnp.int32, (owned, LANES), 0) + core * owned).astype(jnp.float32)

    def block(q, acc):
        part = recv.at[pl.ds(q * pairs, pairs), :, body]
        pltpu.make_async_copy(part, part, recv_sem.at[q]).wait()
        if paired:
            part = recv.at[pl.ds(q * pairs, pairs), core, head]
            pltpu.make_async_copy(part, part, pass_sem.at[q]).wait()
        label = jnp.sum(recv[pl.ds(q * pairs, pairs), :, slots, :].reshape(pack, width), axis=0, keepdims=True)
        hot = (vertex == label).astype(jnp.bfloat16)
        values = recv[pl.ds(q * pairs, pairs), :, pl.ds(0, slots), :].reshape(pack * slots, width)
        high = values.astype(jnp.bfloat16)
        low = (values - high.astype(jnp.float32)).astype(jnp.bfloat16)
        both = jnp.concatenate([high, low], axis=1)
        return acc + jnp.dot(hot, both, preferred_element_type=jnp.float32)

    acc = block(plane, jnp.zeros((owned, 2 * width), jnp.float32))
    if planes <= 8:
        for i in range(planes - 1):
            acc = block(other(i), acc)
    else:
        acc = lax.fori_loop(0, planes - 1, lambda i, a: block(other(i), a), acc)
    out_ref[...] = (acc[:, :width] + acc[:, width:]) / scale
    sent = stage.at[pl.ds(0, total - 1), body]
    pltpu.make_async_copy(sent, sent, send_sem).wait()
    if paired:
        for count, sem in ((rows, 0), (rows, 1)):
            sent = stage.at[pl.ds(0, count), head]
            pltpu.make_async_copy(sent, sent, tail_sem.at[sem]).wait()


def solution(mesh):
    rows, cols = mesh.shape["row"], mesh.shape["col"]
    total = rows * cols

    def body(messages, dst_local, counts, degrees):
        slots, width = messages.shape[3:]
        owned = degrees.shape[0]
        planes = total // (LANES // slots)
        summed = pl.pallas_call(
            functools.partial(exchange, rows, cols),
            out_shape=pltpu.VMEM((owned, width), jnp.float32),
            in_specs=[
                pl.BlockSpec(memory_space=pl.ANY),
                pl.BlockSpec(memory_space=pl.ANY),
                pl.BlockSpec(memory_space=pl.ANY),
                pl.BlockSpec(memory_space=pl.ANY),
            ],
            out_specs=pl.BlockSpec(memory_space=pltpu.VMEM),
            scratch_shapes=[
                pltpu.VMEM((owned // LANES, LANES), jnp.int32),
                pltpu.VMEM((total, slots + 1, width), jnp.float32),
                pltpu.VMEM((rows, cols, slots + 1, width), jnp.float32),
                pltpu.VMEM((total, LANES), jnp.float32),
                pltpu.VMEM(dst_local.shape, jnp.int32),
                pltpu.VMEM((cols, rows), jnp.int32),
                pltpu.VMEM((total, slots // 2, width), jnp.float32),
                pltpu.SemaphoreType.DMA((5,)),
                pltpu.SemaphoreType.DMA,
                pltpu.SemaphoreType.DMA((planes,)),
                pltpu.SemaphoreType.REGULAR((planes,)),
                pltpu.SemaphoreType.DMA((planes,)),
                pltpu.SemaphoreType.DMA((planes,)),
                pltpu.SemaphoreType.DMA((2,)),
            ],
            compiler_params=pltpu.CompilerParams(collective_id=0, has_side_effects=True),
        )(messages.reshape(total, slots, width), dst_local, counts[0].T, degrees.reshape(-1, LANES))
        return summed

    in_specs = (
        P(("row", "col"), None, None, None, None),
        P(("row", "col"), None, None, None),
        P(("row", "col"), None, None),
        P(("row", "col")),
    )
    return jax.shard_map(body, mesh=mesh, in_specs=in_specs, out_specs=P(("row", "col"), None), check_vma=False)
```

```python
import functools

import jax
import jax.numpy as jnp
from jax import lax
from jax.experimental import pallas as pl
from jax.experimental.pallas import tpu as pltpu
from jax.sharding import PartitionSpec as P

MESH = pl.DeviceIdType.MESH
LANES = 128


def exchange(rows, cols, msg_ref, dst_ref, cnt_ref, deg_ref, out_ref, deg, stage, recv, labels, dst, cnt, spare, copy_sem, send_sem, recv_sem, up_sem, extra_sem, pass_sem, tail_sem):
    slots, width = msg_ref.shape[1:]
    owned = out_ref.shape[0]
    total = rows * cols
    pack = LANES // slots
    planes = total // pack
    me = lax.axis_index("row") * cols + lax.axis_index("col")
    plane, seat = me // pack, me % pack
    core = lax.axis_index("col")
    paired = cols == 2 and slots % 16 == 0
    cut = slots // 2 if paired else 0
    pairs = pack // cols

    def device(t):
        return (t // cols, t % cols)

    def repeat(first, last, visit):
        if last - first <= 8:
            for i in range(first, last):
                visit(i)
        else:
            lax.fori_loop(first, last, lambda i, c: (visit(i), c)[1], 0)

    loads = [
        pltpu.make_async_copy(dst_ref, dst, copy_sem.at[0]),
        pltpu.make_async_copy(cnt_ref, cnt, copy_sem.at[1]),
        pltpu.make_async_copy(deg_ref, deg, copy_sem.at[3]),
        pltpu.make_async_copy(msg_ref.at[:, pl.ds(0, slots - cut)], stage.at[:, pl.ds(cut, slots - cut), :], copy_sem.at[2]),
    ]
    if paired:
        loads.append(pltpu.make_async_copy(msg_ref.at[:, pl.ds(cut, cut)], spare, copy_sem.at[4]))
    for load in loads:
        load.start()
    barrier = pltpu.get_barrier_semaphore()

    def greet(t):
        pl.semaphore_signal(barrier, inc=1, device_id=device(t), device_id_type=MESH)

    def greet_above(d):
        @pl.when(plane + d < planes)
        def _():
            repeat(0, pack, lambda j: greet((plane + d) * pack + (seat + j) % pack))

    repeat(1, pack, lambda j: greet(plane * pack + (seat + j) % pack))
    repeat(1, planes, greet_above)
    labels[...] = jnp.zeros_like(labels)
    loads[0].wait()
    loads[1].wait()

    lane = lax.broadcasted_iota(jnp.int32, (cols, slots), 1)
    base = lax.broadcasted_iota(jnp.int32, (cols, slots), 0) * owned
    for g in range(rows):
        value = jnp.where(lane < cnt[:, g : g + 1], dst[0, g] + base, -1).astype(jnp.float32)
        if paired:
            second = cnt[1:2, g : g + 1] > cnt[0:1, g : g + 1]
            extra = jnp.where(second, value[1:2, cut:], value[0:1, cut:])
            labels[pl.ds(g * cols, cols), pl.ds(0, cut)] = jnp.broadcast_to(extra, (cols, cut))
            labels[pl.ds(g * cols, cols), pl.ds(cut, cut)] = value[:, :cut]
        else:
            labels[pl.ds(g * cols, cols), pl.ds(0, slots)] = value
    stage[:, slots, :] = pltpu.roll(labels[...], seat * slots, 1)
    loads[2].wait()
    loads[3].wait()
    if paired:
        loads[4].wait()
        for g in range(rows):
            second = cnt[1:2, g : g + 1] > cnt[0:1, g : g + 1]
            stage[g, pl.ds(0, cut), :] = jnp.where(second, spare[g * cols + 1], spare[g * cols])
    size = deg.shape[1]
    same = lax.broadcasted_iota(jnp.int32, (size, size), 0) == lax.broadcasted_iota(jnp.int32, (size, size), 1)
    scale = jnp.concatenate(
        [jnp.sum(jnp.where(same, jnp.maximum(deg[i : i + 1, :], 1), 0).astype(jnp.float32), axis=1, keepdims=True) for i in range(deg.shape[0])],
        axis=0,
    )

    body = pl.ds(cut, slots + 1 - cut)
    head = pl.ds(0, cut)

    def send(t):
        pltpu.make_async_remote_copy(
            src_ref=stage.at[t, body],
            dst_ref=recv.at[me // cols, core, body],
            send_sem=send_sem,
            recv_sem=recv_sem.at[plane],
            device_id=device(t),
            device_id_type=MESH,
        ).start()

    def send_extra(g):
        pltpu.make_async_remote_copy(
            src_ref=stage.at[g, head],
            dst_ref=recv.at[me // cols, core, head],
            send_sem=tail_sem.at[0],
            recv_sem=extra_sem.at[plane],
            device_id=(g, 1 - core),
            device_id_type=MESH,
        ).start()

    def send_plane(q):
        def send_chip(j):
            if paired:
                send_extra(q * pairs + j)
            for c in range(cols):
                send(q * pack + j * cols + c)

        repeat(0, pairs, send_chip)

    pl.semaphore_wait(barrier, pack - 1 + pack * plane)

    def tell_below(d):
        @pl.when(plane - d >= 0)
        def _():
            t = me - d * pack
            pl.semaphore_signal(up_sem.at[plane], inc=1, device_id=device(t), device_id_type=MESH)

    def send_below(i):
        d = planes - i

        @pl.when(plane - d >= 0)
        def _():
            send_plane(plane - d)

    def send_above(d):
        @pl.when(plane + d < planes)
        def _():
            pl.semaphore_wait(up_sem.at[plane + d], 1)
            send_plane(plane + d)

    repeat(1, planes, tell_below)
    repeat(1, planes, send_below)
    if paired:
        repeat(0, pairs, lambda j: send_extra(plane * pairs + (seat // cols + j) % pairs))
    repeat(1, pack, lambda j: send(plane * pack + (seat + j) % pack))
    pltpu.make_async_copy(stage.at[me, body], recv.at[me // cols, core, body], recv_sem.at[plane]).start()
    repeat(1, planes, send_above)

    def other(i):
        lower = (planes + plane - 1 - i) // planes
        return lower * (plane - 1 - i) + (1 - lower) * (i + 1)

    def hand(q):
        part = recv.at[pl.ds(q * pairs, pairs), 1 - core, head]
        pltpu.make_async_copy(part, part, extra_sem.at[q]).wait()
        pltpu.make_async_remote_copy(
            src_ref=part,
            dst_ref=part,
            send_sem=tail_sem.at[1],
            recv_sem=pass_sem.at[q],
            device_id=(lax.axis_index("row"), 1 - core),
            device_id_type=MESH,
        ).start()

    if paired:
        hand(plane)
        repeat(0, planes - 1, lambda i: hand(other(i)))

    vertex = (lax.broadcasted_iota(jnp.int32, (owned, LANES), 0) + core * owned).astype(jnp.float32)

    def block(q, acc):
        part = recv.at[pl.ds(q * pairs, pairs), :, body]
        pltpu.make_async_copy(part, part, recv_sem.at[q]).wait()
        if paired:
            part = recv.at[pl.ds(q * pairs, pairs), core, head]
            pltpu.make_async_copy(part, part, pass_sem.at[q]).wait()
        label = jnp.sum(recv[pl.ds(q * pairs, pairs), :, slots, :].reshape(pack, width), axis=0, keepdims=True)
        hot = (vertex == label).astype(jnp.bfloat16)
        values = recv[pl.ds(q * pairs, pairs), :, pl.ds(0, slots), :].reshape(pack * slots, width)
        high = values.astype(jnp.bfloat16)
        low = (values - high.astype(jnp.float32)).astype(jnp.bfloat16)
        both = jnp.concatenate([high, low], axis=1)
        return acc + jnp.dot(hot, both, preferred_element_type=jnp.float32)

    acc = block(plane, jnp.zeros((owned, 2 * width), jnp.float32))
    if planes <= 8:
        for i in range(planes - 1):
            acc = block(other(i), acc)
    else:
        acc = lax.fori_loop(0, planes - 1, lambda i, a: block(other(i), a), acc)
    out_ref[...] = (acc[:, :width] + acc[:, width:]) / scale
    sent = stage.at[pl.ds(0, total - 1), body]
    pltpu.make_async_copy(sent, sent, send_sem).wait()
    if paired:
        for count, sem in ((rows, 0), (rows, 1)):
            sent = stage.at[pl.ds(0, count), head]
            pltpu.make_async_copy(sent, sent, tail_sem.at[sem]).wait()


def solution(mesh):
    rows, cols = mesh.shape["row"], mesh.shape["col"]
    total = rows * cols

    def body(messages, dst_local, counts, degrees):
        slots, width = messages.shape[3:]
        owned = degrees.shape[0]
        planes = total // (LANES // slots)
        summed = pl.pallas_call(
            functools.partial(exchange, rows, cols),
            out_shape=pltpu.VMEM((owned, width), jnp.float32),
            in_specs=[
                pl.BlockSpec(memory_space=pl.ANY),
                pl.BlockSpec(memory_space=pl.ANY),
                pl.BlockSpec(memory_space=pl.ANY),
                pl.BlockSpec(memory_space=pl.ANY),
            ],
            out_specs=pl.BlockSpec(memory_space=pltpu.VMEM),
            scratch_shapes=[
                pltpu.VMEM((owned // LANES, LANES), jnp.int32),
                pltpu.VMEM((total, slots + 1, width), jnp.float32),
                pltpu.VMEM((rows, cols, slots + 1, width), jnp.float32),
                pltpu.VMEM((total, LANES), jnp.float32),
                pltpu.VMEM(dst_local.shape, jnp.int32),
                pltpu.VMEM((cols, rows), jnp.int32),
                pltpu.VMEM((total, slots // 2, width), jnp.float32),
                pltpu.SemaphoreType.DMA((5,)),
                pltpu.SemaphoreType.DMA,
                pltpu.SemaphoreType.DMA((planes,)),
                pltpu.SemaphoreType.REGULAR((planes,)),
                pltpu.SemaphoreType.DMA((planes,)),
                pltpu.SemaphoreType.DMA((planes,)),
                pltpu.SemaphoreType.DMA((2,)),
            ],
            compiler_params=pltpu.CompilerParams(collective_id=0, has_side_effects=True),
        )(messages.reshape(total, slots, width), dst_local, counts[0].T, degrees.reshape(-1, LANES))
        return summed

    in_specs = (
        P(("row", "col"), None, None, None, None),
        P(("row", "col"), None, None, None),
        P(("row", "col"), None, None),
        P(("row", "col")),
    )
    return jax.shard_map(body, mesh=mesh, in_specs=in_specs, out_specs=P(("row", "col"), None), check_vma=False)
```
